8 devices in a mesh: frag: 1 (over z), dev: 8 (over y, x, core).
Axes of the slice: x: 2, y: 2, z: 1, core: 2. Of those that a mesh axis runs over, the one named last changes fastest.
Arguments:
- ao_ints: bfloat16 [152, 152, 152, 152], P(('frag', 'dev'))
- occ_coef: bfloat16 [152, 33], P('frag')
- virt_coef: bfloat16 [152, 104], P('frag')
Outputs:
- output: float32 [33, 104, 3432], P('frag', None, 'dev')
All inputs are finite; a program needn't handle non-finite values.
Results may differ from the reference program's by a relative error of at most 0.001.
Values are sent between devices in bfloat16 or wider.
A program may use at most 1 GiB of HBM per device.

```python
import jax
import jax.numpy as jnp
from jax import lax

AO_DIM = 152
OCC_DIM = 33
VIRT_DIM = 104


def setup_inputs(seed: int = 0, part: int = 0) -> dict:
    base_key = jax.random.fold_in(jax.random.key(seed), part)
    key_ints, key_occ, key_virt = jax.random.split(base_key, 3)
    row_keys = jax.random.split(key_ints, AO_DIM)

    def draw_row(row_key):
        return jax.random.normal(row_key, (AO_DIM, AO_DIM, AO_DIM), jnp.float32).astype(jnp.bfloat16)

    ao_ints = lax.map(draw_row, row_keys)
    coef_scale = AO_DIM ** -0.5
    occ_coef = jax.random.normal(key_occ, (AO_DIM, OCC_DIM), jnp.float32) * coef_scale
    virt_coef = jax.random.normal(key_virt, (AO_DIM, VIRT_DIM), jnp.float32) * coef_scale
    return {"ao_ints": ao_ints, "occ_coef": occ_coef.astype(jnp.bfloat16), "virt_coef": virt_coef.astype(jnp.bfloat16)}


def reference(ao_ints, occ_coef, virt_coef):
    occ_wide = occ_coef.astype(jnp.float32)
    virt_wide = virt_coef.astype(jnp.float32)

    def first_half(ao_row):
        quarter = jnp.einsum("qrs,rj->qsj", ao_row.astype(jnp.float32), occ_wide).astype(jnp.bfloat16)
        half_row = jnp.einsum("qsj,sb->qjb", quarter.astype(jnp.float32), virt_wide).astype(jnp.bfloat16)
        return half_row.reshape(AO_DIM, OCC_DIM * VIRT_DIM)

    half_ints = lax.map(first_half, ao_ints)
    three_quarter = jnp.einsum("qa,pqc->apc", virt_wide, half_ints.astype(jnp.float32)).astype(jnp.bfloat16)
    return jnp.einsum("pi,apc->iac", occ_wide, three_quarter.astype(jnp.float32))
```

```python
import functools

import jax
import jax.numpy as jnp
from jax import lax
from jax.experimental import pallas as pl
from jax.experimental.pallas import tpu as pltpu
from jax.sharding import PartitionSpec as P

F32 = jnp.float32
BF16 = jnp.bfloat16
AO, OCC, VIRT = 152, 33, 104
DEVS = 8
ROWS = AO // DEVS
PAIRS = OCC * VIRT // DEVS
PITCH = 40
CHUNK = 19
CHUNKS = AO // CHUNK
SLOTS = 8
BLK = 3 * VIRT + 56
LANES = 128


def _exchange_kernel(a_hbm, cot_ref, cv_ref, g_out, abuf, cot, cvp, cvt, ts0, ts1, gsend, asem, ssem, rsem, lsem):
    me = lax.axis_index("dev")

    def a_copy(n):
        return pltpu.make_async_copy(
            a_hbm.at[n // CHUNKS, pl.ds(lax.rem(n, CHUNKS) * CHUNK, CHUNK)],
            abuf.at[lax.rem(n, SLOTS)],
            asem.at[lax.rem(n, SLOTS)],
        )

    for n in range(SLOTS):
        a_copy(n).start()

    barrier = pltpu.get_barrier_semaphore()
    for k in range(1, DEVS):
        pl.semaphore_signal(
            barrier, inc=1, device_id={"dev": lax.rem(me + k, DEVS)}, device_id_type=pl.DeviceIdType.MESH
        )

    cot[...] = jnp.zeros_like(cot)
    cot[0:OCC, :] = cot_ref[...]
    cvp[...] = jnp.zeros_like(cvp)
    cvp[0:AO, 0:VIRT] = cv_ref[...]
    cvt[...] = cvp[...].astype(F32).T[0:VIRT, :].astype(BF16)
    ts1[...] = jnp.zeros_like(ts1)

    pl.semaphore_wait(barrier, DEVS - 1)

    lane = lax.broadcasted_iota(jnp.int32, (VIRT, LANES), 1)
    lane56 = lax.broadcasted_iota(jnp.int32, (56, LANES), 1)

    def send(row, d):
        @pl.when(d != me)
        def _():
            pltpu.make_async_remote_copy(
                src_ref=gsend.at[row, d],
                dst_ref=g_out.at[me * ROWS + row],
                send_sem=ssem.at[row, d],
                recv_sem=rsem.at[row, me],
                device_id={"dev": d},
                device_id_type=pl.DeviceIdType.MESH,
            ).start()

        @pl.when(d == me)
        def _():
            pltpu.make_async_copy(gsend.at[row, d], g_out.at[me * ROWS + row], lsem.at[row]).start()

    def row_body(row, carry):
        def chunk_body(c, carry):
            n = row * CHUNKS + c
            slot = lax.rem(n, SLOTS)
            a_copy(n).wait()
            for u in range(CHUNK):
                t = jnp.dot(cot[...], abuf[slot, u], preferred_element_type=F32)
                base = pl.multiple_of((c * CHUNK + u) * PITCH, 8)
                ts0[pl.ds(base, PITCH), :] = t[:, 0:LANES]
                ts1[pl.ds(base, PITCH), 0 : AO - LANES] = t[:, LANES:AO]

            @pl.when(n + SLOTS < ROWS * CHUNKS)
            def _():
                a_copy(n + SLOTS).start()

            return carry

        lax.fori_loop(0, CHUNKS, chunk_body, 0)

        g = {}

        def half(j):
            lhs = jnp.concatenate(
                [ts0[pl.ds(j, AO, stride=PITCH), :], ts1[pl.ds(j, AO, stride=PITCH), :]], axis=1
            ).astype(BF16)
            return jnp.dot(lhs, cvp[...], preferred_element_type=F32).astype(BF16)

        def need(j):
            if j in g:
                return
            if j + 1 < OCC:
                h = jnp.concatenate([half(j), half(j + 1)], axis=1)
                both = jnp.dot(cvt[:, 0:AO], h, preferred_element_type=F32)
                g[j], g[j + 1] = both[:, 0:LANES], both[:, LANES : 2 * LANES]
            else:
                g[j] = jnp.dot(cvt[:, 0:AO], half(j), preferred_element_type=F32)

        for d in range(DEVS):
            first = PAIRS * d
            j0, j1 = first // VIRT, (first + PAIRS - 1) // VIRT
            rolled = {}
            for j in range(j0, j1 + 1):
                need(j)
                shift = (VIRT * j - first) % LANES
                rolled[j] = pltpu.roll(g[j], shift, axis=1) if shift else g[j]
            tiles = []
            for t in range(4):
                lo = first + LANES * t
                hi = min(lo + LANES, first + PAIRS)
                ja, jb = lo // VIRT, (hi - 1) // VIRT
                tile = rolled[ja]
                for j in range(ja + 1, jb + 1):
                    tile = jnp.where(lane >= VIRT * j - lo, rolled[j], tile)
                tiles.append(tile)
            last = tiles.pop()
            tiles.append(jnp.where(lane56 < 64, last[0:56], pltpu.roll(last[48:VIRT], 64, axis=1)))
            gsend[row, d] = jnp.concatenate(tiles, axis=0).astype(BF16)
            if d:
                send(row, d - 1)
        send(row, DEVS - 1)
        return carry

    lax.fori_loop(0, ROWS, row_body, 0)

    def drain(row, carry):
        for k in range(DEVS):
            @pl.when(k != me)
            def _():
                pltpu.make_async_remote_copy(
                    src_ref=gsend.at[row, k],
                    dst_ref=g_out.at[k * ROWS + row],
                    send_sem=ssem.at[row, k],
                    recv_sem=rsem.at[row, k],
                    device_id={"dev": k},
                    device_id_type=pl.DeviceIdType.MESH,
                ).wait()

        pltpu.make_async_copy(gsend.at[row, 0], g_out.at[me * ROWS + row], lsem.at[row]).wait()
        return carry

    lax.fori_loop(0, ROWS, drain, 0)


def _exchange(ao_rows, cot, cv):
    return pl.pallas_call(
        _exchange_kernel,
        out_shape=jax.ShapeDtypeStruct((AO, BLK, LANES), BF16),
        in_specs=[
            pl.BlockSpec(memory_space=pl.ANY),
            pl.BlockSpec(memory_space=pltpu.VMEM),
            pl.BlockSpec(memory_space=pltpu.VMEM),
        ],
        out_specs=pl.BlockSpec(memory_space=pl.ANY),
        scratch_shapes=[
            pltpu.VMEM((SLOTS, CHUNK, AO, AO), BF16),
            pltpu.VMEM((PITCH, AO), BF16),
            pltpu.VMEM((2 * LANES, LANES), BF16),
            pltpu.VMEM((VIRT, 2 * LANES), BF16),
            pltpu.VMEM((AO * PITCH, LANES), F32),
            pltpu.VMEM((AO * PITCH, LANES), F32),
            pltpu.VMEM((ROWS, DEVS, BLK, LANES), BF16),
            pltpu.SemaphoreType.DMA((SLOTS,)),
            pltpu.SemaphoreType.DMA((ROWS, DEVS)),
            pltpu.SemaphoreType.DMA((ROWS, DEVS)),
            pltpu.SemaphoreType.DMA((ROWS,)),
        ],
        compiler_params=pltpu.CompilerParams(
            collective_id=0, has_side_effects=True, vmem_limit_bytes=62 * 1024 * 1024
        ),
        name="exchange",
    )(ao_rows, cot, cv)


def _last_kernel(lhs_ref, g_ref, out_ref):
    step = pl.program_id(0)
    x = g_ref[...].astype(F32)
    low = x[:, 0:8, :].reshape(AO * 8, LANES)
    high = x[:, 8:16, :].reshape(AO * 8, LANES)
    rhs = jnp.concatenate([low, high], axis=1).astype(BF16)
    v = jnp.dot(lhs_ref[...], rhs, preferred_element_type=F32)
    for u in range(2):
        part = v[:, u * LANES : (u + 1) * LANES].reshape(OCC, 8, LANES)
        m = 2 * step + u

        @pl.when(m < 39)
        def _():
            rows = pl.ds(pl.multiple_of(lax.rem(m, 13) * 8, 8), 8)
            cols = pl.ds(pl.multiple_of(m // 13 * LANES, LANES), LANES)
            out_ref[:, rows, cols] = part

        @pl.when(m >= 39)
        def _():
            k = (m - 39) * 8
            out_ref[:, pl.ds(pl.multiple_of(k, 8), 8), 384:PAIRS] = part[:, :, 0 : PAIRS - 384]

        @pl.when(m >= 40)
        def _():
            k = (m - 39) * 8 + 48
            moved = pltpu.roll(part, 64, axis=2)
            out_ref[:, pl.ds(pl.multiple_of(k, 8), 8), 384:PAIRS] = moved[:, :, 0 : PAIRS - 384]


def _last(lhs, g):
    return pl.pallas_call(
        _last_kernel,
        grid=(BLK // 16,),
        out_shape=jax.ShapeDtypeStruct((OCC, VIRT, PAIRS), F32),
        in_specs=[
            pl.BlockSpec((OCC * 8, AO * 8), lambda s: (0, 0)),
            pl.BlockSpec((AO, 16, LANES), lambda s: (0, s, 0)),
        ],
        out_specs=pl.BlockSpec((OCC, VIRT, PAIRS), lambda s: (0, 0, 0)),
        compiler_params=pltpu.CompilerParams(vmem_limit_bytes=50 * 1024 * 1024),
        name="last",
    )(lhs, g)


def solution(mesh):
    def local_part(ao_rows, occ_coef, virt_coef):
        g = _exchange(ao_rows, occ_coef.T, virt_coef)
        lhs = jnp.kron(occ_coef.T, jnp.eye(8, dtype=BF16))
        return _last(lhs, g)

    return jax.shard_map(
        local_part,
        mesh=mesh,
        in_specs=(P(("frag", "dev"), None, None, None), P("frag", None), P("frag", None)),
        out_specs=P("frag", None, "dev"),
        check_vma=False,
    )
```

```python
import functools

import jax
import jax.numpy as jnp
from jax import lax
from jax.experimental import pallas as pl
from jax.experimental.pallas import tpu as pltpu
from jax.sharding import PartitionSpec as P

F32 = jnp.float32
BF16 = jnp.bfloat16
AO, OCC, VIRT = 152, 33, 104
DEVS = 8
ROWS = AO // DEVS
PAIRS = OCC * VIRT // DEVS
PITCH = 40
CHUNK = 19
CHUNKS = AO // CHUNK
SLOTS = 6
LANES = 128
TILES = VIRT // 8
REST = PAIRS - 3 * LANES
RTILES = -(-TILES * REST // LANES)
BLK = 8 * (3 * TILES + RTILES)
EARLY = 16
LATE = ROWS - EARLY


def _step4(lhs_ref, load, put, rest, lane8):
    depth = lhs_ref.shape[1]

    def group(g):
        return load(g).reshape(depth, LANES)

    def product(groups):
        rhs = jnp.concatenate([group(g) for g in groups], axis=1)
        return jnp.dot(lhs_ref[...], rhs, preferred_element_type=F32).reshape(OCC, 16, len(groups) * LANES)

    def tile(v, m):
        g, u = divmod(m, 2)
        return v[:, 8 * u : 8 * u + 8, g * LANES : (g + 1) * LANES]

    base = 18
    v = product([base + k for k in range(BLK // 16 - base)])
    tail = [tile(v, k) for k in range(3)]
    packed = [tile(v, 3 + k) for k in range(RTILES)]
    for n in range(TILES):
        start = REST * n
        k0, k1 = start // LANES, (start + REST - 1) // LANES
        back = (-start) % LANES
        piece = pltpu.roll(packed[k0], back, axis=2) if back else packed[k0]
        if k1 != k0:
            other = pltpu.roll(packed[k1], back, axis=2)
            piece = jnp.where(lane8 < LANES * k1 - start, piece, other)
        rest[:, 8 * n : 8 * n + 8, :] = piece

    def pair(e, carry):
        v = product([3 * e, 3 * e + 1, 3 * e + 2])
        put(e, 2, [tile(v, m) for m in range(6)])
        return carry

    lax.fori_loop(0, TILES // 2, pair, 0)
    put(TILES // 2, 1, tail)


def _spread(cot_f32, width, owner):
    k = lax.broadcasted_iota(jnp.int32, (AO, width), 1)
    p = lax.broadcasted_iota(jnp.int32, (AO, width), 0)
    pick = jnp.where(p == owner(k // 16), 1.0, 0.0).astype(BF16)
    wide = jnp.dot(cot_f32, pick, preferred_element_type=F32)[0:OCC]
    a = lax.broadcasted_iota(jnp.int32, (16, width), 0)
    ka = lax.rem(lax.broadcasted_iota(jnp.int32, (16, width), 1), 16)
    keep = (a == ka)[None]
    return jnp.where(keep, wide[:, None, :], 0.0).reshape(OCC * 16, width).astype(BF16)


def _exchange_kernel(
    a_hbm, cot_ref, cv_ref, v_out, g_out, lhs_out,
    abuf, cot, cvp, cvt, ts0, ts1, gsend, grecv, vacc, rest, lhs, late,
    asem, ssem, rsem, lsem, vsem, hsem,
):
    me = lax.axis_index("dev")

    def a_copy(n):
        return pltpu.make_async_copy(
            a_hbm.at[n // CHUNKS, pl.ds(lax.rem(n, CHUNKS) * CHUNK, CHUNK)],
            abuf.at[lax.rem(n, SLOTS)],
            asem.at[lax.rem(n, SLOTS)],
        )

    for n in range(SLOTS):
        a_copy(n).start()

    barrier = pltpu.get_barrier_semaphore()
    for k in range(1, DEVS):
        pl.semaphore_signal(
            barrier, inc=1, device_id={"dev": lax.rem(me + k, DEVS)}, device_id_type=pl.DeviceIdType.MESH
        )

    cot[...] = jnp.zeros_like(cot)
    cot[0:OCC, :] = cot_ref[...]
    cvp[...] = jnp.zeros_like(cvp)
    cvp[0:AO, 0:VIRT] = cv_ref[...]
    cvt[...] = cvp[...].astype(F32).T[0:VIRT, :].astype(BF16)
    ts1[...] = jnp.zeros_like(ts1)

    pl.semaphore_wait(barrier, DEVS - 1)

    lane = lax.broadcasted_iota(jnp.int32, (VIRT, LANES), 1)
    lane8 = lax.broadcasted_iota(jnp.int32, (8, LANES), 1)

    def early_copy(row, src, dst):
        return pltpu.make_async_remote_copy(
            src_ref=gsend.at[row, dst],
            dst_ref=grecv.at[src * EARLY + row],
            send_sem=ssem.at[row, dst],
            recv_sem=rsem.at[row, src],
            device_id={"dev": dst},
            device_id_type=pl.DeviceIdType.MESH,
        )

    def late_copy(row, src, dst):
        return pltpu.make_async_remote_copy(
            src_ref=gsend.at[row, dst],
            dst_ref=g_out.at[src * LATE + row - EARLY],
            send_sem=ssem.at[row, dst],
            recv_sem=rsem.at[row, src],
            device_id={"dev": dst},
            device_id_type=pl.DeviceIdType.MESH,
        )

    def own_copy(row):
        return pltpu.make_async_copy(gsend.at[row, me], g_out.at[me * LATE + row - EARLY], lsem.at[row - EARLY])

    def send(row, d):
        @pl.when((d != me) & (row < EARLY))
        def _():
            early_copy(row, me, d).start()

        @pl.when((d != me) & (row >= EARLY))
        def _():
            late_copy(row, me, d).start()

        @pl.when((d == me) & (row < EARLY))
        def _():
            grecv[me * EARLY + row] = gsend[row, d]

        @pl.when((d == me) & (row >= EARLY))
        def _():
            own_copy(row).start()

    def row_body(row, carry):
        def chunk_body(c, carry):
            n = row * CHUNKS + c
            slot = lax.rem(n, SLOTS)
            a_copy(n).wait()
            for u in range(CHUNK):
                t = jnp.dot(cot[...], abuf[slot, u], preferred_element_type=F32)
                base = pl.multiple_of((c * CHUNK + u) * PITCH, 8)
                ts0[pl.ds(base, PITCH), :] = t[:, 0:LANES]
                ts1[pl.ds(base, PITCH), 0 : AO - LANES] = t[:, LANES:AO]

            @pl.when(n + SLOTS < ROWS * CHUNKS)
            def _():
                a_copy(n + SLOTS).start()

            return carry

        lax.fori_loop(0, CHUNKS, chunk_body, 0)

        g = {}

        def half(j):
            lhs = jnp.concatenate(
                [ts0[pl.ds(j, AO, stride=PITCH), :], ts1[pl.ds(j, AO, stride=PITCH), :]], axis=1
            ).astype(BF16)
            return jnp.dot(lhs, cvp[...], preferred_element_type=F32).astype(BF16)

        def need(j):
            if j in g:
                return
            if j + 1 < OCC:
                h = jnp.concatenate([half(j), half(j + 1)], axis=1)
                both = jnp.dot(cvt[:, 0:AO], h, preferred_element_type=F32)
                g[j], g[j + 1] = both[:, 0:LANES], both[:, LANES : 2 * LANES]
            else:
                g[j] = jnp.dot(cvt[:, 0:AO], half(j), preferred_element_type=F32)

        for d in range(DEVS):
            first = PAIRS * d
            j0, j1 = first // VIRT, (first + PAIRS - 1) // VIRT
            rolled = {}
            for j in range(j0, j1 + 1):
                need(j)
                shift = (VIRT * j - first) % LANES
                rolled[j] = pltpu.roll(g[j], shift, axis=1) if shift else g[j]
            tiles = []
            for t in range(4):
                lo = first + LANES * t
                hi = min(lo + LANES, first + PAIRS)
                ja, jb = lo // VIRT, (hi - 1) // VIRT
                tile = rolled[ja]
                for j in range(ja + 1, jb + 1):
                    tile = jnp.where(lane >= VIRT * j - lo, rolled[j], tile)
                tiles.append(tile)
            last = tiles.pop()
            parts = [tile[8 * n : 8 * n + 8] for n in range(TILES) for tile in tiles]
            moved = []
            for n in range(TILES):
                shift = REST * n % LANES
                piece = last[8 * n : 8 * n + 8]
                moved.append(pltpu.roll(piece, shift, axis=1) if shift else piece)
            for k in range(RTILES):
                n0, n1 = LANES * k // REST, min((LANES * k + LANES - 1) // REST, TILES - 1)
                part = moved[n0]
                for n in range(n0 + 1, n1 + 1):
                    part = jnp.where(lane8 >= REST * n - LANES * k, moved[n], part)
                parts.append(part)
            gsend[row, d] = jnp.concatenate(parts, axis=0).astype(BF16)
            if d:
                send(row, d - 1)
        send(row, DEVS - 1)
        return carry

    lax.fori_loop(0, ROWS, row_body, 0)

    vacc[...] = jnp.zeros_like(vacc)
    for s in range(DEVS):
        cols = slice(s * EARLY * 16, (s + 1) * EARLY * 16)
        lhs[:, cols] = _spread(cot[...], EARLY * 16, lambda q: s * ROWS + q)
    late[...] = _spread(cot[...], DEVS * LATE * 16, lambda q: q // LATE * ROWS + EARLY + lax.rem(q, LATE))
    late_out = pltpu.make_async_copy(late, lhs_out, hsem)
    late_out.start()

    def arrived(row, carry):
        for k in range(DEVS):
            @pl.when(k != me)
            def _():
                early_copy(row, k, me).wait_recv()

        return carry

    lax.fori_loop(0, EARLY, arrived, 0)

    def v_copy(e, width):
        rows = pl.ds(pl.multiple_of(e * 16, 8), 8 * width)
        return pltpu.make_async_copy(vacc.at[:, rows, :], v_out.at[:, rows, :], vsem.at[e])

    def put(e, width, tiles):
        for w in range(width):
            rows = pl.ds(pl.multiple_of(e * 16 + 8 * w, 8), 8)
            for t in range(3):
                vacc[:, rows, t * LANES : (t + 1) * LANES] += tiles[3 * w + t]
            vacc[:, rows, 3 * LANES : PAIRS] = rest[:, rows, 0:REST]
        v_copy(e, width).start()

    def load(g):
        return grecv[:, pl.ds(pl.multiple_of(g * 16, 16), 16), :]

    _step4(lhs, load, put, rest, lane8)

    def arrived_late(row, carry):
        for k in range(DEVS):
            @pl.when(k != me)
            def _():
                late_copy(row, k, me).wait_recv()

        own_copy(row).wait()
        return carry

    lax.fori_loop(EARLY, ROWS, arrived_late, 0)

    def sent(row, carry):
        for k in range(DEVS):
            @pl.when(k != me)
            def _():
                pltpu.make_async_remote_copy(
                    src_ref=gsend.at[row, k],
                    dst_ref=g_out.at[0],
                    send_sem=ssem.at[row, k],
                    recv_sem=rsem.at[row, k],
                    device_id={"dev": k},
                    device_id_type=pl.DeviceIdType.MESH,
                ).wait_send()

        return carry

    lax.fori_loop(0, ROWS, sent, 0)

    def stored(e, carry):
        v_copy(e, 2).wait()
        return carry

    lax.fori_loop(0, TILES // 2, stored, 0)
    v_copy(TILES // 2, 1).wait()
    late_out.wait()


def _exchange(ao_rows, cot, cv):
    return pl.pallas_call(
        _exchange_kernel,
        out_shape=(
            jax.ShapeDtypeStruct((OCC, VIRT, PAIRS), F32),
            jax.ShapeDtypeStruct((DEVS * LATE, BLK, LANES), BF16),
            jax.ShapeDtypeStruct((OCC * 16, DEVS * LATE * 16), BF16),
        ),
        in_specs=[
            pl.BlockSpec(memory_space=pl.ANY),
            pl.BlockSpec(memory_space=pltpu.VMEM),
            pl.BlockSpec(memory_space=pltpu.VMEM),
        ],
        out_specs=tuple(pl.BlockSpec(memory_space=pl.ANY) for _ in range(3)),
        scratch_shapes=[
            pltpu.VMEM((SLOTS, CHUNK, AO, AO), BF16),
            pltpu.VMEM((PITCH, AO), BF16),
            pltpu.VMEM((2 * LANES, LANES), BF16),
            pltpu.VMEM((VIRT, 2 * LANES), BF16),
            pltpu.VMEM((AO * PITCH, LANES), F32),
            pltpu.VMEM((AO * PITCH, LANES), F32),
            pltpu.VMEM((ROWS, DEVS, BLK, LANES), BF16),
            pltpu.VMEM((DEVS * EARLY, BLK, LANES), BF16),
            pltpu.VMEM((OCC, VIRT, PAIRS), F32),
            pltpu.VMEM((OCC, VIRT, LANES), F32),
            pltpu.VMEM((OCC * 16, DEVS * EARLY * 16), BF16),
            pltpu.VMEM((OCC * 16, DEVS * LATE * 16), BF16),
            pltpu.SemaphoreType.DMA((SLOTS,)),
            pltpu.SemaphoreType.DMA((ROWS, DEVS)),
            pltpu.SemaphoreType.DMA((ROWS, DEVS)),
            pltpu.SemaphoreType.DMA((LATE,)),
            pltpu.SemaphoreType.DMA((TILES // 2 + 1,)),
            pltpu.SemaphoreType.DMA,
        ],
        compiler_params=pltpu.CompilerParams(
            collective_id=0, has_side_effects=True, vmem_limit_bytes=63 * 1024 * 1024
        ),
        name="exchange",
    )(ao_rows, cot, cv)


def _last_kernel(lhs_ref, g_ref, v_hbm, out_hbm, vbuf, rest, isem, osem):
    lane8 = lax.broadcasted_iota(jnp.int32, (8, LANES), 1)

    def part(e, width, ref, into, sem):
        rows = pl.ds(pl.multiple_of(e * 16, 8), 8 * width)
        src, dst = ref.at[:, rows, :], vbuf.at[:, rows, :]
        return pltpu.make_async_copy(src, dst, sem.at[e]) if into else pltpu.make_async_copy(dst, src, sem.at[e])

    for e in range(TILES // 2):
        part(e, 2, v_hbm, True, isem).start()
    part(TILES // 2, 1, v_hbm, True, isem).start()

    def put(e, width, tiles):
        part(e, width, v_hbm, True, isem).wait()
        for w in range(width):
            rows = pl.ds(pl.multiple_of(e * 16 + 8 * w, 8), 8)
            for t in range(3):
                vbuf[:, rows, t * LANES : (t + 1) * LANES] += tiles[3 * w + t]
            vbuf[:, rows, 3 * LANES : PAIRS] += rest[:, rows, 0:REST]
        part(e, width, out_hbm, False, osem).start()

    def load(g):
        return g_ref[:, pl.ds(pl.multiple_of(g * 16, 16), 16), :]

    _step4(lhs_ref, load, put, rest, lane8)

    for e in range(TILES // 2):
        part(e, 2, out_hbm, False, osem).wait()
    part(TILES // 2, 1, out_hbm, False, osem).wait()


def _last(lhs, g, v):
    return pl.pallas_call(
        _last_kernel,
        out_shape=jax.ShapeDtypeStruct((OCC, VIRT, PAIRS), F32),
        in_specs=[
            pl.BlockSpec(memory_space=pltpu.VMEM),
            pl.BlockSpec(memory_space=pltpu.VMEM),
            pl.BlockSpec(memory_space=pl.ANY),
        ],
        out_specs=pl.BlockSpec(memory_space=pl.ANY),
        scratch_shapes=[
            pltpu.VMEM((OCC, VIRT, PAIRS), F32),
            pltpu.VMEM((OCC, VIRT, LANES), F32),
            pltpu.SemaphoreType.DMA((TILES // 2 + 1,)),
            pltpu.SemaphoreType.DMA((TILES // 2 + 1,)),
        ],
        compiler_params=pltpu.CompilerParams(vmem_limit_bytes=50 * 1024 * 1024),
        name="last",
    )(lhs, g, v)


def solution(mesh):
    def local_part(ao_rows, occ_coef, virt_coef):
        v, g, lhs = _exchange(ao_rows, occ_coef.T, virt_coef)
        return _last(lhs, g, v)

    return jax.shard_map(
        local_part,
        mesh=mesh,
        in_specs=(P(("frag", "dev"), None, None, None), P("frag", None), P("frag", None)),
        out_specs=P("frag", None, "dev"),
        check_vma=False,
    )
```

```python
import functools

import jax
import jax.numpy as jnp
from jax import lax
from jax.experimental import pallas as pl
from jax.experimental.pallas import tpu as pltpu
from jax.sharding import PartitionSpec as P

F32 = jnp.float32
BF16 = jnp.bfloat16
AO, OCC, VIRT = 152, 33, 104
DEVS = 8
ROWS = AO // DEVS
PAIRS = OCC * VIRT // DEVS
PITCH = 40
CHUNK = 19
CHUNKS = AO // CHUNK
SLOTS = 6
LANES = 128
TILES = VIRT // 8
REST = PAIRS - 3 * LANES
RTILES = -(-TILES * REST // LANES)
BLK = 8 * (3 * TILES + RTILES)
GROUPS = ((0, 1, 2, 3, 4, 5), (6, 7, 8, 9, 10, 11, 12, 13), (14, 15, 16, 17, 18, 19, 20, 21), (22, 23, 24, 25, 26, 27, 28, 29, 30, 31, 32))
EARLY = 16
LATE = ROWS - EARLY


def _step4(lhs_ref, load, put, rest, lane8):
    depth = lhs_ref.shape[1]

    def group(g):
        return load(g).reshape(depth, LANES)

    def product(groups):
        rhs = jnp.concatenate([group(g) for g in groups], axis=1)
        return jnp.dot(lhs_ref[...], rhs, preferred_element_type=F32).reshape(OCC, 16, len(groups) * LANES)

    def tile(v, m):
        g, u = divmod(m, 2)
        return v[:, 8 * u : 8 * u + 8, g * LANES : (g + 1) * LANES]

    base = 18
    v = product([base + k for k in range(BLK // 16 - base)])
    tail = [tile(v, k) for k in range(3)]
    packed = [tile(v, 3 + k) for k in range(RTILES)]
    for n in range(TILES):
        start = REST * n
        k0, k1 = start // LANES, (start + REST - 1) // LANES
        back = (-start) % LANES
        piece = pltpu.roll(packed[k0], back, axis=2) if back else packed[k0]
        if k1 != k0:
            other = pltpu.roll(packed[k1], back, axis=2)
            piece = jnp.where(lane8 < LANES * k1 - start, piece, other)
        rest[:, 8 * n : 8 * n + 8, :] = piece

    def pair(e, carry):
        v = product([3 * e, 3 * e + 1, 3 * e + 2])
        put(e, 2, [tile(v, m) for m in range(6)])
        return carry

    lax.fori_loop(0, TILES // 2, pair, 0)
    put(TILES // 2, 1, tail)


def _spread(cot_f32, width, owner):
    k = lax.broadcasted_iota(jnp.int32, (AO, width), 1)
    p = lax.broadcasted_iota(jnp.int32, (AO, width), 0)
    pick = jnp.where(p == owner(k // 16), 1.0, 0.0).astype(BF16)
    wide = jnp.dot(cot_f32, pick, preferred_element_type=F32)[0:OCC]
    a = lax.broadcasted_iota(jnp.int32, (16, width), 0)
    ka = lax.rem(lax.broadcasted_iota(jnp.int32, (16, width), 1), 16)
    keep = (a == ka)[None]
    return jnp.where(keep, wide[:, None, :], 0.0).reshape(OCC * 16, width).astype(BF16)


def _exchange_kernel(
    a_hbm, cot_ref, cv_ref, v_out, g_out, lhs_out,
    abuf, cot, cvp, cvt, ts0, ts1, gsend, grecv, vacc, rest, lhs, late,
    asem, ssem, rsem, lsem, vsem, hsem,
):
    me = lax.axis_index("dev")

    def a_copy(n):
        return pltpu.make_async_copy(
            a_hbm.at[n // CHUNKS, pl.ds(lax.rem(n, CHUNKS) * CHUNK, CHUNK)],
            abuf.at[lax.rem(n, SLOTS)],
            asem.at[lax.rem(n, SLOTS)],
        )

    for n in range(SLOTS):
        a_copy(n).start()

    barrier = pltpu.get_barrier_semaphore()
    for k in range(1, DEVS):
        pl.semaphore_signal(
            barrier, inc=1, device_id={"dev": lax.rem(me + k, DEVS)}, device_id_type=pl.DeviceIdType.MESH
        )

    cot[...] = jnp.zeros_like(cot)
    cot[0:OCC, :] = cot_ref[...]
    cvp[...] = jnp.zeros_like(cvp)
    cvp[:, 0:VIRT] = cv_ref[...]
    square = jnp.concatenate([cvp[...].astype(F32), jnp.zeros((2 * LANES - AO, LANES), F32)], axis=0)
    cvt[...] = square.T[0:VIRT, 0:AO].astype(BF16)

    pl.semaphore_wait(barrier, DEVS - 1)

    lane = lax.broadcasted_iota(jnp.int32, (VIRT, LANES), 1)
    lane8 = lax.broadcasted_iota(jnp.int32, (8, LANES), 1)

    def early_copy(row, src, dst):
        return pltpu.make_async_remote_copy(
            src_ref=gsend.at[row, dst],
            dst_ref=grecv.at[src * EARLY + row],
            send_sem=ssem.at[row, dst],
            recv_sem=rsem.at[row, src],
            device_id={"dev": dst},
            device_id_type=pl.DeviceIdType.MESH,
        )

    def late_copy(row, src, dst):
        return pltpu.make_async_remote_copy(
            src_ref=gsend.at[row, dst],
            dst_ref=g_out.at[src * LATE + row - EARLY],
            send_sem=ssem.at[row, dst],
            recv_sem=rsem.at[row, src],
            device_id={"dev": dst},
            device_id_type=pl.DeviceIdType.MESH,
        )

    def own_copy(row):
        return pltpu.make_async_copy(gsend.at[row, me], g_out.at[me * LATE + row - EARLY], lsem.at[row - EARLY])

    def send(row, d):
        @pl.when((d != me) & (row < EARLY))
        def _():
            early_copy(row, me, d).start()

        @pl.when((d != me) & (row >= EARLY))
        def _():
            late_copy(row, me, d).start()

        @pl.when((d == me) & (row < EARLY))
        def _():
            grecv[me * EARLY + row] = gsend[row, d]

        @pl.when((d == me) & (row >= EARLY))
        def _():
            own_copy(row).start()

    def row_body(row, carry):
        def chunk_body(c, carry):
            n = row * CHUNKS + c
            slot = lax.rem(n, SLOTS)
            a_copy(n).wait()
            for u in range(CHUNK):
                t = jnp.dot(cot[...], abuf[slot, u], preferred_element_type=F32)
                base = pl.multiple_of((c * CHUNK + u) * PITCH, 8)
                ts0[pl.ds(base, PITCH), :] = t[:, 0:LANES]
                ts1[pl.ds(base, PITCH), 0 : AO - LANES] = t[:, LANES:AO]

            @pl.when(n + SLOTS < ROWS * CHUNKS)
            def _():
                a_copy(n + SLOTS).start()

            return carry

        lax.fori_loop(0, CHUNKS, chunk_body, 0)

        g = {}

        def need(j):
            if j in g:
                return
            group = next(js for js in GROUPS if j in js)
            lhs = jnp.concatenate(
                [
                    jnp.concatenate([(ts0, ts1)[k][pl.ds(jj, AO, stride=PITCH), :] for jj in group], axis=0)
                    for k in range(2)
                ],
                axis=1,
            )
            lhs = lhs[:, 0:AO].astype(BF16)
            half = jnp.dot(lhs, cvp[...], preferred_element_type=F32)
            wide = jnp.concatenate([half[AO * n : AO * n + AO] for n in range(len(group))], axis=1).astype(BF16)
            full = jnp.dot(cvt[...], wide, preferred_element_type=F32)
            for n, jj in enumerate(group):
                g[jj] = full[:, LANES * n : LANES * n + LANES]

        for d in range(DEVS):
            first = PAIRS * d
            j0, j1 = first // VIRT, (first + PAIRS - 1) // VIRT
            rolled = {}
            for j in range(j0, j1 + 1):
                need(j)
                shift = (VIRT * j - first) % LANES
                rolled[j] = pltpu.roll(g[j], shift, axis=1) if shift else g[j]
            tiles = []
            for t in range(4):
                lo = first + LANES * t
                hi = min(lo + LANES, first + PAIRS)
                ja, jb = lo // VIRT, (hi - 1) // VIRT
                tile = rolled[ja]
                for j in range(ja + 1, jb + 1):
                    tile = jnp.where(lane >= VIRT * j - lo, rolled[j], tile)
                tiles.append(tile)
            last = tiles.pop()
            parts = [tile[8 * n : 8 * n + 8] for n in range(TILES) for tile in tiles]
            moved = []
            for n in range(TILES):
                shift = REST * n % LANES
                piece = last[8 * n : 8 * n + 8]
                moved.append(pltpu.roll(piece, shift, axis=1) if shift else piece)
            for k in range(RTILES):
                n0, n1 = LANES * k // REST, min((LANES * k + LANES - 1) // REST, TILES - 1)
                part = moved[n0]
                for n in range(n0 + 1, n1 + 1):
                    part = jnp.where(lane8 >= REST * n - LANES * k, moved[n], part)
                parts.append(part)
            gsend[row, d] = jnp.concatenate(parts, axis=0).astype(BF16)
            if d:
                send(row, d - 1)
        send(row, DEVS - 1)
        return carry

    lax.fori_loop(0, ROWS, row_body, 0)

    vacc[...] = jnp.zeros_like(vacc)
    for s in range(DEVS):
        cols = slice(s * EARLY * 16, (s + 1) * EARLY * 16)
        lhs[:, cols] = _spread(cot[...], EARLY * 16, lambda q: s * ROWS + q)
    late[...] = _spread(cot[...], DEVS * LATE * 16, lambda q: q // LATE * ROWS + EARLY + lax.rem(q, LATE))
    late_out = pltpu.make_async_copy(late, lhs_out, hsem)
    late_out.start()

    def arrived(row, carry):
        for k in range(DEVS):
            @pl.when(k != me)
            def _():
                early_copy(row, k, me).wait_recv()

        return carry

    lax.fori_loop(0, EARLY, arrived, 0)

    def v_copy(e, width):
        rows = pl.ds(pl.multiple_of(e * 16, 8), 8 * width)
        return pltpu.make_async_copy(vacc.at[:, rows, :], v_out.at[:, rows, :], vsem.at[e])

    def put(e, width, tiles):
        for w in range(width):
            rows = pl.ds(pl.multiple_of(e * 16 + 8 * w, 8), 8)
            for t in range(3):
                vacc[:, rows, t * LANES : (t + 1) * LANES] += tiles[3 * w + t]
            vacc[:, rows, 3 * LANES : PAIRS] = rest[:, rows, 0:REST]
        v_copy(e, width).start()

    def load(g):
        return grecv[:, pl.ds(pl.multiple_of(g * 16, 16), 16), :]

    _step4(lhs, load, put, rest, lane8)

    def arrived_late(row, carry):
        for k in range(DEVS):
            @pl.when(k != me)
            def _():
                late_copy(row, k, me).wait_recv()

        own_copy(row).wait()
        return carry

    lax.fori_loop(EARLY, ROWS, arrived_late, 0)

    def sent(row, carry):
        for k in range(DEVS):
            @pl.when(k != me)
            def _():
                pltpu.make_async_remote_copy(
                    src_ref=gsend.at[row, k],
                    dst_ref=g_out.at[0],
                    send_sem=ssem.at[row, k],
                    recv_sem=rsem.at[row, k],
                    device_id={"dev": k},
                    device_id_type=pl.DeviceIdType.MESH,
                ).wait_send()

        return carry

    lax.fori_loop(0, ROWS, sent, 0)

    def stored(e, carry):
        v_copy(e, 2).wait()
        return carry

    lax.fori_loop(0, TILES // 2, stored, 0)
    v_copy(TILES // 2, 1).wait()
    late_out.wait()


def _exchange(ao_rows, cot, cv):
    return pl.pallas_call(
        _exchange_kernel,
        out_shape=(
            jax.ShapeDtypeStruct((OCC, VIRT, PAIRS), F32),
            jax.ShapeDtypeStruct((DEVS * LATE, BLK, LANES), BF16),
            jax.ShapeDtypeStruct((OCC * 16, DEVS * LATE * 16), BF16),
        ),
        in_specs=[
            pl.BlockSpec(memory_space=pl.ANY),
            pl.BlockSpec(memory_space=pltpu.VMEM),
            pl.BlockSpec(memory_space=pltpu.VMEM),
        ],
        out_specs=tuple(pl.BlockSpec(memory_space=pl.ANY) for _ in range(3)),
        scratch_shapes=[
            pltpu.VMEM((SLOTS, CHUNK, AO, AO), BF16),
            pltpu.VMEM((PITCH, AO), BF16),
            pltpu.VMEM((AO, LANES), BF16),
            pltpu.VMEM((VIRT, AO), BF16),
            pltpu.VMEM((AO * PITCH, LANES), F32),
            pltpu.VMEM((AO * PITCH, LANES), F32),
            pltpu.VMEM((ROWS, DEVS, BLK, LANES), BF16),
            pltpu.VMEM((DEVS * EARLY, BLK, LANES), BF16),
            pltpu.VMEM((OCC, VIRT, PAIRS), F32),
            pltpu.VMEM((OCC, VIRT, LANES), F32),
            pltpu.VMEM((OCC * 16, DEVS * EARLY * 16), BF16),
            pltpu.VMEM((OCC * 16, DEVS * LATE * 16), BF16),
            pltpu.SemaphoreType.DMA((SLOTS,)),
            pltpu.SemaphoreType.DMA((ROWS, DEVS)),
            pltpu.SemaphoreType.DMA((ROWS, DEVS)),
            pltpu.SemaphoreType.DMA((LATE,)),
            pltpu.SemaphoreType.DMA((TILES // 2 + 1,)),
            pltpu.SemaphoreType.DMA,
        ],
        compiler_params=pltpu.CompilerParams(
            collective_id=0, has_side_effects=True, vmem_limit_bytes=63 * 1024 * 1024
        ),
        name="exchange",
    )(ao_rows, cot, cv)


def _last_kernel(lhs_ref, g_ref, v_hbm, out_hbm, vbuf, rest, isem, osem):
    lane8 = lax.broadcasted_iota(jnp.int32, (8, LANES), 1)

    def part(e, width, ref, into, sem):
        rows = pl.ds(pl.multiple_of(e * 16, 8), 8 * width)
        src, dst = ref.at[:, rows, :], vbuf.at[:, rows, :]
        return pltpu.make_async_copy(src, dst, sem.at[e]) if into else pltpu.make_async_copy(dst, src, sem.at[e])

    for e in range(TILES // 2):
        part(e, 2, v_hbm, True, isem).start()
    part(TILES // 2, 1, v_hbm, True, isem).start()

    def put(e, width, tiles):
        part(e, width, v_hbm, True, isem).wait()
        for w in range(width):
            rows = pl.ds(pl.multiple_of(e * 16 + 8 * w, 8), 8)
            for t in range(3):
                vbuf[:, rows, t * LANES : (t + 1) * LANES] += tiles[3 * w + t]
            vbuf[:, rows, 3 * LANES : PAIRS] += rest[:, rows, 0:REST]
        part(e, width, out_hbm, False, osem).start()

    def load(g):
        return g_ref[:, pl.ds(pl.multiple_of(g * 16, 16), 16), :]

    _step4(lhs_ref, load, put, rest, lane8)

    for e in range(TILES // 2):
        part(e, 2, out_hbm, False, osem).wait()
    part(TILES // 2, 1, out_hbm, False, osem).wait()


def _last(lhs, g, v):
    return pl.pallas_call(
        _last_kernel,
        out_shape=jax.ShapeDtypeStruct((OCC, VIRT, PAIRS), F32),
        in_specs=[
            pl.BlockSpec(memory_space=pltpu.VMEM),
            pl.BlockSpec(memory_space=pltpu.VMEM),
            pl.BlockSpec(memory_space=pl.ANY),
        ],
        out_specs=pl.BlockSpec(memory_space=pl.ANY),
        scratch_shapes=[
            pltpu.VMEM((OCC, VIRT, PAIRS), F32),
            pltpu.VMEM((OCC, VIRT, LANES), F32),
            pltpu.SemaphoreType.DMA((TILES // 2 + 1,)),
            pltpu.SemaphoreType.DMA((TILES // 2 + 1,)),
        ],
        compiler_params=pltpu.CompilerParams(vmem_limit_bytes=50 * 1024 * 1024),
        name="last",
    )(lhs, g, v)


def solution(mesh):
    def local_part(ao_rows, occ_coef, virt_coef):
        v, g, lhs = _exchange(ao_rows, occ_coef.T, virt_coef)
        return _last(lhs, g, v)

    return jax.shard_map(
        local_part,
        mesh=mesh,
        in_specs=(P(("frag", "dev"), None, None, None), P("frag", None), P("frag", None)),
        out_specs=P("frag", None, "dev"),
        check_vma=False,
    )
```

```python
import functools

import jax
import jax.numpy as jnp
from jax import lax
from jax.experimental import pallas as pl
from jax.experimental.pallas import tpu as pltpu
from jax.sharding import PartitionSpec as P

F32 = jnp.float32
BF16 = jnp.bfloat16
AO, OCC, VIRT = 152, 33, 104
DEVS = 8
ROWS = AO // DEVS
PAIRS = OCC * VIRT // DEVS
PITCH = 40
CHUNK = 19
CHUNKS = AO // CHUNK
SLOTS = 4
RING = 10
LANES = 128
TILES = VIRT // 8
REST = PAIRS - 3 * LANES
RTILES = -(-TILES * REST // LANES)
BLK = 8 * (3 * TILES + RTILES)
GROUPS = ((0, 1, 2, 3, 4, 5), (6, 7, 8, 9, 10, 11, 12, 13), (14, 15, 16, 17, 18, 19, 20, 21), (22, 23, 24, 25, 26, 27, 28, 29, 30, 31, 32))
EARLY = 17
LATE = ROWS - EARLY


def _step4(lhs_ref, load, put, rest, lane8, unroll):
    depth = lhs_ref.shape[1]

    def group(g):
        return load(g).reshape(depth, LANES)

    def product(groups):
        rhs = jnp.concatenate([group(g) for g in groups], axis=1)
        return jnp.dot(lhs_ref[...], rhs, preferred_element_type=F32).reshape(OCC, 16, len(groups) * LANES)

    def tile(v, m):
        g, u = divmod(m, 2)
        return v[:, 8 * u : 8 * u + 8, g * LANES : (g + 1) * LANES]

    base = 18
    v = product([base + k for k in range(BLK // 16 - base)])
    tail = [tile(v, k) for k in range(3)]
    packed = [tile(v, 3 + k) for k in range(RTILES)]
    for n in range(TILES):
        start = REST * n
        k0, k1 = start // LANES, (start + REST - 1) // LANES
        back = (-start) % LANES
        piece = pltpu.roll(packed[k0], back, axis=2) if back else packed[k0]
        if k1 != k0:
            other = pltpu.roll(packed[k1], back, axis=2)
            piece = jnp.where(lane8 < LANES * k1 - start, piece, other)
        rest[:, 8 * n : 8 * n + 8, :] = piece

    def pair(e, carry):
        v = product([3 * e, 3 * e + 1, 3 * e + 2])
        put(e, 2, [tile(v, m) for m in range(6)])
        return carry

    if unroll:
        for e in range(TILES // 2):
            pair(e, 0)
    else:
        lax.fori_loop(0, TILES // 2, pair, 0)
    put(TILES // 2, 1, tail)


def _spread(cot_f32, width, owner):
    k = lax.broadcasted_iota(jnp.int32, (AO, width), 1)
    p = lax.broadcasted_iota(jnp.int32, (AO, width), 0)
    pick = jnp.where(p == owner(k // 16), 1.0, 0.0).astype(BF16)
    wide = jnp.dot(cot_f32, pick, preferred_element_type=F32)[0:OCC]
    a = lax.broadcasted_iota(jnp.int32, (16, width), 0)
    ka = lax.rem(lax.broadcasted_iota(jnp.int32, (16, width), 1), 16)
    keep = (a == ka)[None]
    return jnp.where(keep, wide[:, None, :], 0.0).reshape(OCC * 16, width).astype(BF16)


def _exchange_kernel(
    a_hbm, cot_ref, cv_ref, v_out, g_out, lhs_out,
    abuf, cot, cvp, cvt, ts0, ts1, gsend, grecv, rest, lhs,
    asem, ssem, rsem,
):
    me = lax.axis_index("dev")

    def a_copy(n):
        return pltpu.make_async_copy(
            a_hbm.at[n // CHUNKS, pl.ds(lax.rem(n, CHUNKS) * CHUNK, CHUNK)],
            abuf.at[lax.rem(n, SLOTS)],
            asem.at[lax.rem(n, SLOTS)],
        )

    for n in range(SLOTS):
        a_copy(n).start()

    barrier = pltpu.get_barrier_semaphore()
    for k in range(1, DEVS):
        pl.semaphore_signal(
            barrier, inc=1, device_id={"dev": lax.rem(me + k, DEVS)}, device_id_type=pl.DeviceIdType.MESH
        )

    cot[...] = jnp.zeros_like(cot)
    cot[0:OCC, :] = cot_ref[...]
    cvp[...] = jnp.zeros_like(cvp)
    cvp[:, 0:VIRT] = cv_ref[...]
    square = jnp.concatenate([cvp[...].astype(F32), jnp.zeros((2 * LANES - AO, LANES), F32)], axis=0)
    cvt[...] = square.T[0:VIRT, 0:AO].astype(BF16)

    lane = lax.broadcasted_iota(jnp.int32, (VIRT, LANES), 1)
    lane8 = lax.broadcasted_iota(jnp.int32, (8, LANES), 1)

    def early_copy(row, src, dst):
        return pltpu.make_async_remote_copy(
            src_ref=gsend.at[lax.rem(row, RING), dst],
            dst_ref=grecv.at[src * EARLY + row],
            send_sem=ssem.at[row, dst],
            recv_sem=rsem.at[row, src],
            device_id={"dev": dst},
            device_id_type=pl.DeviceIdType.MESH,
        )

    def late_copy(row, src, dst, sems=None):
        sems = row if sems is None else sems
        return pltpu.make_async_remote_copy(
            src_ref=gsend.at[lax.rem(row, RING), dst],
            dst_ref=g_out.at[src * LATE + row - EARLY],
            send_sem=ssem.at[sems, dst],
            recv_sem=rsem.at[sems, src],
            device_id={"dev": dst},
            device_id_type=pl.DeviceIdType.MESH,
        )

    def send(row, d):
        @pl.when((d != me) & (row < EARLY))
        def _():
            early_copy(row, me, d).start()

        @pl.when((d != me) & (row >= EARLY))
        def _():
            late_copy(row, me, d).start()

        @pl.when((d == me) & (row < EARLY))
        def _():
            grecv[me * EARLY + row] = gsend[lax.rem(row, RING), d]

        @pl.when((d == me) & (row >= EARLY))
        def _():
            g_out[me * LATE + row - EARLY] = gsend[lax.rem(row, RING), d]

    def sent(row):
        for k in range(DEVS):
            @pl.when(k != me)
            def _():
                late_copy(EARLY, me, k, row).wait_send()

    def row_body(row, carry):
        def chunk_body(c, carry):
            n = row * CHUNKS + c
            slot = lax.rem(n, SLOTS)
            a_copy(n).wait()
            for u in range(CHUNK):
                t = jnp.dot(cot[...], abuf[slot, u], preferred_element_type=F32)
                base = pl.multiple_of((c * CHUNK + u) * PITCH, 8)
                ts0[pl.ds(base, PITCH), :] = t[:, 0:LANES]
                ts1[pl.ds(base, PITCH), 0 : AO - LANES] = t[:, LANES:AO]

            @pl.when(n + SLOTS < ROWS * CHUNKS)
            def _():
                a_copy(n + SLOTS).start()

            return carry

        lax.fori_loop(0, CHUNKS, chunk_body, 0)

        @pl.when(row == 0)
        def _():
            pl.semaphore_wait(barrier, DEVS - 1)

        @pl.when(row >= RING)
        def _():
            sent(row - RING)


        g = {}

        def need(j):
            if j in g:
                return
            group = next(js for js in GROUPS if j in js)
            lhs = jnp.concatenate(
                [
                    jnp.concatenate([(ts0, ts1)[k][pl.ds(jj, AO, stride=PITCH), :] for jj in group], axis=0)
                    for k in range(2)
                ],
                axis=1,
            )
            lhs = lhs[:, 0:AO].astype(BF16)
            half = jnp.dot(lhs, cvp[...], preferred_element_type=F32)
            wide = jnp.concatenate([half[AO * n : AO * n + AO] for n in range(len(group))], axis=1).astype(BF16)
            full = jnp.dot(cvt[...], wide, preferred_element_type=F32)
            for n, jj in enumerate(group):
                g[jj] = full[:, LANES * n : LANES * n + LANES]

        for d in range(DEVS):
            first = PAIRS * d
            j0, j1 = first // VIRT, (first + PAIRS - 1) // VIRT
            rolled = {}
            for j in range(j0, j1 + 1):
                need(j)
                shift = (VIRT * j - first) % LANES
                rolled[j] = pltpu.roll(g[j], shift, axis=1) if shift else g[j]
            tiles = []
            for t in range(4):
                lo = first + LANES * t
                hi = min(lo + LANES, first + PAIRS)
                ja, jb = lo // VIRT, (hi - 1) // VIRT
                tile = rolled[ja]
                for j in range(ja + 1, jb + 1):
                    tile = jnp.where(lane >= VIRT * j - lo, rolled[j], tile)
                tiles.append(tile)
            last = tiles.pop()
            parts = [tile[8 * n : 8 * n + 8] for n in range(TILES) for tile in tiles]
            moved = []
            for n in range(TILES):
                shift = REST * n % LANES
                piece = last[8 * n : 8 * n + 8]
                moved.append(pltpu.roll(piece, shift, axis=1) if shift else piece)
            for k in range(RTILES):
                n0, n1 = LANES * k // REST, min((LANES * k + LANES - 1) // REST, TILES - 1)
                part = moved[n0]
                for n in range(n0 + 1, n1 + 1):
                    part = jnp.where(lane8 >= REST * n - LANES * k, moved[n], part)
                parts.append(part)
            gsend[lax.rem(row, RING), d] = jnp.concatenate(parts, axis=0).astype(BF16)
            if d:
                send(row, d - 1)
        send(row, DEVS - 1)
        return carry

    lax.fori_loop(0, ROWS, row_body, 0)

    v_out[...] = jnp.zeros_like(v_out)
    for s in range(DEVS):
        cols = slice(s * EARLY * 16, (s + 1) * EARLY * 16)
        lhs[:, cols] = _spread(cot[...], EARLY * 16, lambda q: s * ROWS + q)
    lhs_out[...] = _spread(cot[...], DEVS * LATE * 16, lambda q: q // LATE * ROWS + EARLY + lax.rem(q, LATE))

    def arrived(row, carry):
        for k in range(DEVS):
            @pl.when(k != me)
            def _():
                early_copy(row, k, me).wait_recv()

        return carry

    lax.fori_loop(0, EARLY, arrived, 0)

    def put(e, width, tiles):
        for w in range(width):
            rows = pl.ds(pl.multiple_of(e * 16 + 8 * w, 8), 8)
            for t in range(3):
                v_out[:, rows, t * LANES : (t + 1) * LANES] += tiles[3 * w + t]
            v_out[:, rows, 3 * LANES : PAIRS] = rest[:, rows, 0:REST]

    def load(g):
        return grecv[:, pl.ds(pl.multiple_of(g * 16, 16), 16), :]

    _step4(lhs, load, put, rest, lane8, False)

    def arrived_late(row, carry):
        for k in range(DEVS):
            @pl.when(k != me)
            def _():
                late_copy(row, k, me).wait_recv()

        return carry

    lax.fori_loop(EARLY, ROWS, arrived_late, 0)

    lax.fori_loop(ROWS - RING, ROWS, lambda row, carry: sent(row) or carry, 0)


def _exchange(ao_rows, cot, cv):
    return pl.pallas_call(
        _exchange_kernel,
        out_shape=(
            jax.ShapeDtypeStruct((OCC, VIRT, PAIRS), F32),
            jax.ShapeDtypeStruct((DEVS * LATE, BLK, LANES), BF16),
            jax.ShapeDtypeStruct((OCC * 16, DEVS * LATE * 16), BF16),
        ),
        in_specs=[pl.BlockSpec(memory_space=pl.ANY)] + [pl.BlockSpec(memory_space=pltpu.VMEM)] * 2,
        out_specs=tuple(pl.BlockSpec(memory_space=pltpu.VMEM) for _ in range(3)),
        scratch_shapes=[
            pltpu.VMEM((SLOTS, CHUNK, AO, AO), BF16),
            pltpu.VMEM((PITCH, AO), BF16),
            pltpu.VMEM((AO, LANES), BF16),
            pltpu.VMEM((VIRT, AO), BF16),
            pltpu.VMEM((AO * PITCH, LANES), F32),
            pltpu.VMEM((AO * PITCH, LANES), F32),
            pltpu.VMEM((RING, DEVS, BLK, LANES), BF16),
            pltpu.VMEM((DEVS * EARLY, BLK, LANES), BF16),
            pltpu.VMEM((OCC, VIRT, LANES), F32),
            pltpu.VMEM((OCC * 16, DEVS * EARLY * 16), BF16),
            pltpu.SemaphoreType.DMA((SLOTS,)),
            pltpu.SemaphoreType.DMA((ROWS, DEVS)),
            pltpu.SemaphoreType.DMA((ROWS, DEVS)),
        ],
        compiler_params=pltpu.CompilerParams(
            collective_id=0, has_side_effects=True, vmem_limit_bytes=38 * 1024 * 1024
        ),
        name="exchange",
    )(ao_rows, cot, cv)


def _last_kernel(lhs_ref, g_ref, v_ref, out_hbm, vbuf, rest, osem):
    lane8 = lax.broadcasted_iota(jnp.int32, (8, LANES), 1)

    def part(e, width):
        rows = pl.ds(pl.multiple_of(e * 16, 8), 8 * width)
        return pltpu.make_async_copy(vbuf.at[:, rows, :], out_hbm.at[:, rows, :], osem.at[e])

    def put(e, width, tiles):
        for w in range(width):
            rows = pl.ds(pl.multiple_of(e * 16 + 8 * w, 8), 8)
            for t in range(3):
                vbuf[:, rows, t * LANES : (t + 1) * LANES] = v_ref[:, rows, t * LANES : (t + 1) * LANES] + tiles[3 * w + t]
            vbuf[:, rows, 3 * LANES : PAIRS] = v_ref[:, rows, 3 * LANES : PAIRS] + rest[:, rows, 0:REST]
        part(e, width).start()

    def load(g):
        return g_ref[:, pl.ds(pl.multiple_of(g * 16, 16), 16), :]

    _step4(lhs_ref, load, put, rest, lane8, True)

    for e in range(TILES // 2):
        part(e, 2).wait()
    part(TILES // 2, 1).wait()


def _last(lhs, g, v):
    return pl.pallas_call(
        _last_kernel,
        out_shape=jax.ShapeDtypeStruct((OCC, VIRT, PAIRS), F32),
        in_specs=[
            pl.BlockSpec(memory_space=pltpu.VMEM),
            pl.BlockSpec(memory_space=pltpu.VMEM),
            pl.BlockSpec(memory_space=pltpu.VMEM),
        ],
        out_specs=pl.BlockSpec(memory_space=pl.ANY),
        scratch_shapes=[
            pltpu.VMEM((OCC, VIRT, PAIRS), F32),
            pltpu.VMEM((OCC, VIRT, LANES), F32),
            pltpu.SemaphoreType.DMA((TILES // 2 + 1,)),
        ],
        compiler_params=pltpu.CompilerParams(vmem_limit_bytes=30 * 1024 * 1024),
        name="last",
    )(lhs, g, v)


def solution(mesh):
    def local_part(ao_rows, occ_coef, virt_coef):
        v, g, lhs = _exchange(ao_rows, occ_coef.T, virt_coef)
        return _last(lhs, g, v)

    return jax.shard_map(
        local_part,
        mesh=mesh,
        in_specs=(P(("frag", "dev"), None, None, None), P("frag", None), P("frag", None)),
        out_specs=P("frag", None, "dev"),
        check_vma=False,
    )
```

```python
import functools

import jax
import jax.numpy as jnp
from jax import lax
from jax.experimental import pallas as pl
from jax.experimental.pallas import tpu as pltpu
from jax.sharding import PartitionSpec as P

F32 = jnp.float32
BF16 = jnp.bfloat16
AO, OCC, VIRT = 152, 33, 104
DEVS = 8
ROWS = AO // DEVS
PAIRS = OCC * VIRT // DEVS
PITCH = 40
CHUNK = 19
CHUNKS = AO // CHUNK
SLOTS = 4
RING = 10
LANES = 128
TILES = VIRT // 8
REST = PAIRS - 3 * LANES
RTILES = -(-TILES * REST // LANES)
BLK = 8 * (3 * TILES + RTILES)
GROUPS = ((0, 1, 2, 3, 4, 5), (6, 7, 8, 9, 10, 11, 12, 13), (14, 15, 16, 17, 18, 19, 20, 21), (22, 23, 24, 25, 26, 27, 28, 29, 30, 31, 32))
EARLY = 17
LATE = ROWS - EARLY


def _step4(lhs_ref, load, put, rest, lane8, unroll):
    depth = lhs_ref.shape[1]

    def group(g):
        return load(g).reshape(depth, LANES)

    def product(groups):
        rhs = jnp.concatenate([group(g) for g in groups], axis=1)
        return jnp.dot(lhs_ref[...], rhs, preferred_element_type=F32).reshape(OCC, 16, len(groups) * LANES)

    def tile(v, m):
        g, u = divmod(m, 2)
        return v[:, 8 * u : 8 * u + 8, g * LANES : (g + 1) * LANES]

    base = 18
    v = product([base + k for k in range(BLK // 16 - base)])
    tail = [tile(v, k) for k in range(3)]
    packed = [tile(v, 3 + k) for k in range(RTILES)]
    for n in range(TILES):
        start = REST * n
        k0, k1 = start // LANES, (start + REST - 1) // LANES
        back = (-start) % LANES
        piece = pltpu.roll(packed[k0], back, axis=2) if back else packed[k0]
        if k1 != k0:
            other = pltpu.roll(packed[k1], back, axis=2)
            piece = jnp.where(lane8 < LANES * k1 - start, piece, other)
        rest[:, 8 * n : 8 * n + 8, :] = piece

    def pair(e, carry):
        v = product([3 * e, 3 * e + 1, 3 * e + 2])
        put(e, 2, [tile(v, m) for m in range(6)])
        return carry

    if unroll:
        for e in range(TILES // 2):
            pair(e, 0)
    else:
        lax.fori_loop(0, TILES // 2, pair, 0)
    put(TILES // 2, 1, tail)


def _spread(cot_f32, width, owner):
    k = lax.broadcasted_iota(jnp.int32, (AO, width), 1)
    p = lax.broadcasted_iota(jnp.int32, (AO, width), 0)
    pick = jnp.where(p == owner(k // 16), 1.0, 0.0).astype(BF16)
    wide = jnp.dot(cot_f32, pick, preferred_element_type=F32)[0:OCC]
    a = lax.broadcasted_iota(jnp.int32, (16, width), 0)
    ka = lax.rem(lax.broadcasted_iota(jnp.int32, (16, width), 1), 16)
    keep = (a == ka)[None]
    return jnp.where(keep, wide[:, None, :], 0.0).reshape(OCC * 16, width).astype(BF16)


def _exchange_kernel(
    a_hbm, cot_hbm, cv_hbm, v_out, g_out, lhs_out,
    abuf, cot, cvp, cvt, ts0, ts1, gsend, grecv, rest, lhs,
    asem, ssem, rsem, csem, cot_ref, cv_ref,
):
    me = lax.axis_index("dev")

    def a_copy(n):
        return pltpu.make_async_copy(
            a_hbm.at[n // CHUNKS, pl.ds(lax.rem(n, CHUNKS) * CHUNK, CHUNK)],
            abuf.at[lax.rem(n, SLOTS)],
            asem.at[lax.rem(n, SLOTS)],
        )

    cot_copy = pltpu.make_async_copy(cot_hbm, cot_ref, csem.at[0])
    cv_copy = pltpu.make_async_copy(cv_hbm, cv_ref, csem.at[1])
    cot_copy.start()
    cv_copy.start()
    for n in range(SLOTS):
        a_copy(n).start()

    barrier = pltpu.get_barrier_semaphore()
    for k in range(1, DEVS):
        pl.semaphore_signal(
            barrier, inc=1, device_id={"dev": lax.rem(me + k, DEVS)}, device_id_type=pl.DeviceIdType.MESH
        )

    cot_copy.wait()
    cv_copy.wait()
    cot[...] = jnp.zeros_like(cot)
    cot[0:OCC, :] = cot_ref[...]
    cvp[...] = jnp.zeros_like(cvp)
    cvp[:, 0:VIRT] = cv_ref[...]
    square = jnp.concatenate([cvp[...].astype(F32), jnp.zeros((2 * LANES - AO, LANES), F32)], axis=0)
    cvt[...] = square.T[0:VIRT, 0:AO].astype(BF16)

    lane = lax.broadcasted_iota(jnp.int32, (VIRT, LANES), 1)
    lane8 = lax.broadcasted_iota(jnp.int32, (8, LANES), 1)

    def early_copy(row, src, dst):
        return pltpu.make_async_remote_copy(
            src_ref=gsend.at[lax.rem(row, RING), dst],
            dst_ref=grecv.at[src * EARLY + row],
            send_sem=ssem.at[row, dst],
            recv_sem=rsem.at[row, src],
            device_id={"dev": dst},
            device_id_type=pl.DeviceIdType.MESH,
        )

    def late_copy(row, src, dst, sems=None):
        sems = row if sems is None else sems
        return pltpu.make_async_remote_copy(
            src_ref=gsend.at[lax.rem(row, RING), dst],
            dst_ref=g_out.at[src * LATE + row - EARLY],
            send_sem=ssem.at[sems, dst],
            recv_sem=rsem.at[sems, src],
            device_id={"dev": dst},
            device_id_type=pl.DeviceIdType.MESH,
        )

    def send(row, d):
        @pl.when((d != me) & (row < EARLY))
        def _():
            early_copy(row, me, d).start()

        @pl.when((d != me) & (row >= EARLY))
        def _():
            late_copy(row, me, d).start()

        @pl.when((d == me) & (row < EARLY))
        def _():
            grecv[me * EARLY + row] = gsend[lax.rem(row, RING), d]

        @pl.when((d == me) & (row >= EARLY))
        def _():
            g_out[me * LATE + row - EARLY] = gsend[lax.rem(row, RING), d]

    def sent(row):
        for k in range(DEVS):
            @pl.when(k != me)
            def _():
                late_copy(EARLY, me, k, row).wait_send()

    def row_body(row, carry):
        def chunk_body(c, carry):
            n = row * CHUNKS + c
            slot = lax.rem(n, SLOTS)
            a_copy(n).wait()
            for u in range(CHUNK):
                t = jnp.dot(cot[...], abuf[slot, u], preferred_element_type=F32)
                base = pl.multiple_of((c * CHUNK + u) * PITCH, 8)
                ts0[pl.ds(base, PITCH), :] = t[:, 0:LANES]
                ts1[pl.ds(base, PITCH), 0 : AO - LANES] = t[:, LANES:AO]

            @pl.when(n + SLOTS < ROWS * CHUNKS)
            def _():
                a_copy(n + SLOTS).start()

            return carry

        lax.fori_loop(0, CHUNKS, chunk_body, 0)

        @pl.when(row == 0)
        def _():
            pl.semaphore_wait(barrier, DEVS - 1)

        @pl.when(row >= RING)
        def _():
            sent(row - RING)


        g = {}

        def need(j):
            if j in g:
                return
            group = next(js for js in GROUPS if j in js)
            lhs = jnp.concatenate(
                [
                    jnp.concatenate([(ts0, ts1)[k][pl.ds(jj, AO, stride=PITCH), :] for jj in group], axis=0)
                    for k in range(2)
                ],
                axis=1,
            )
            lhs = lhs[:, 0:AO].astype(BF16)
            half = jnp.dot(lhs, cvp[...], preferred_element_type=F32)
            wide = jnp.concatenate([half[AO * n : AO * n + AO] for n in range(len(group))], axis=1).astype(BF16)
            full = jnp.dot(cvt[...], wide, preferred_element_type=F32)
            for n, jj in enumerate(group):
                g[jj] = full[:, LANES * n : LANES * n + LANES]

        for d in range(DEVS):
            first = PAIRS * d
            j0, j1 = first // VIRT, (first + PAIRS - 1) // VIRT
            rolled = {}
            for j in range(j0, j1 + 1):
                need(j)
                shift = (VIRT * j - first) % LANES
                rolled[j] = pltpu.roll(g[j], shift, axis=1) if shift else g[j]
            tiles = []
            for t in range(4):
                lo = first + LANES * t
                hi = min(lo + LANES, first + PAIRS)
                ja, jb = lo // VIRT, (hi - 1) // VIRT
                tile = rolled[ja]
                for j in range(ja + 1, jb + 1):
                    tile = jnp.where(lane >= VIRT * j - lo, rolled[j], tile)
                tiles.append(tile)
            last = tiles.pop()
            parts = [tile[8 * n : 8 * n + 8] for n in range(TILES) for tile in tiles]
            moved = []
            for n in range(TILES):
                shift = REST * n % LANES
                piece = last[8 * n : 8 * n + 8]
                moved.append(pltpu.roll(piece, shift, axis=1) if shift else piece)
            for k in range(RTILES):
                n0, n1 = LANES * k // REST, min((LANES * k + LANES - 1) // REST, TILES - 1)
                part = moved[n0]
                for n in range(n0 + 1, n1 + 1):
                    part = jnp.where(lane8 >= REST * n - LANES * k, moved[n], part)
                parts.append(part)
            gsend[lax.rem(row, RING), d] = jnp.concatenate(parts, axis=0).astype(BF16)
            if d:
                send(row, d - 1)
        send(row, DEVS - 1)
        return carry

    lax.fori_loop(0, ROWS, row_body, 0)

    v_out[...] = jnp.zeros_like(v_out)
    for s in range(DEVS):
        cols = slice(s * EARLY * 16, (s + 1) * EARLY * 16)
        lhs[:, cols] = _spread(cot[...], EARLY * 16, lambda q: s * ROWS + q)
    lhs_out[...] = _spread(cot[...], DEVS * LATE * 16, lambda q: q // LATE * ROWS + EARLY + lax.rem(q, LATE))

    def arrived(row, carry):
        for k in range(DEVS):
            @pl.when(k != me)
            def _():
                early_copy(row, k, me).wait_recv()

        return carry

    lax.fori_loop(0, EARLY, arrived, 0)

    def put(e, width, tiles):
        for w in range(width):
            rows = pl.ds(pl.multiple_of(e * 16 + 8 * w, 8), 8)
            for t in range(3):
                v_out[:, rows, t * LANES : (t + 1) * LANES] += tiles[3 * w + t]
            v_out[:, rows, 3 * LANES : PAIRS] = rest[:, rows, 0:REST]

    def load(g):
        return grecv[:, pl.ds(pl.multiple_of(g * 16, 16), 16), :]

    _step4(lhs, load, put, rest, lane8, False)

    def arrived_late(row, carry):
        for k in range(DEVS):
            @pl.when(k != me)
            def _():
                late_copy(row, k, me).wait_recv()

        return carry

    lax.fori_loop(EARLY, ROWS, arrived_late, 0)

    lax.fori_loop(ROWS - RING, ROWS, lambda row, carry: sent(row) or carry, 0)


def _exchange(ao_rows, cot, cv):
    return pl.pallas_call(
        _exchange_kernel,
        out_shape=(
            jax.ShapeDtypeStruct((OCC, VIRT, PAIRS), F32),
            jax.ShapeDtypeStruct((DEVS * LATE, BLK, LANES), BF16),
            jax.ShapeDtypeStruct((OCC * 16, DEVS * LATE * 16), BF16),
        ),
        in_specs=[pl.BlockSpec(memory_space=pltpu.HBM)] * 3,
        out_specs=tuple(pl.BlockSpec(memory_space=pltpu.VMEM) for _ in range(3)),
        scratch_shapes=[
            pltpu.VMEM((SLOTS, CHUNK, AO, AO), BF16),
            pltpu.VMEM((PITCH, AO), BF16),
            pltpu.VMEM((AO, LANES), BF16),
            pltpu.VMEM((VIRT, AO), BF16),
            pltpu.VMEM((AO * PITCH, LANES), F32),
            pltpu.VMEM((AO * PITCH, LANES), F32),
            pltpu.VMEM((RING, DEVS, BLK, LANES), BF16),
            pltpu.VMEM((DEVS * EARLY, BLK, LANES), BF16),
            pltpu.VMEM((OCC, VIRT, LANES), F32),
            pltpu.VMEM((OCC * 16, DEVS * EARLY * 16), BF16),
            pltpu.SemaphoreType.DMA((SLOTS,)),
            pltpu.SemaphoreType.DMA((ROWS, DEVS)),
            pltpu.SemaphoreType.DMA((ROWS, DEVS)),
            pltpu.SemaphoreType.DMA((2,)),
            pltpu.VMEM((OCC, AO), BF16),
            pltpu.VMEM((AO, VIRT), BF16),
        ],
        compiler_params=pltpu.CompilerParams(
            collective_id=0, has_side_effects=True, vmem_limit_bytes=38 * 1024 * 1024
        ),
        name="exchange",
    )(ao_rows, cot, cv)


def _last_kernel(lhs_ref, g_ref, v_ref, out_hbm, vbuf, rest, osem):
    lane8 = lax.broadcasted_iota(jnp.int32, (8, LANES), 1)

    def part(e, width):
        rows = pl.ds(pl.multiple_of(e * 16, 8), 8 * width)
        return pltpu.make_async_copy(vbuf.at[:, rows, :], out_hbm.at[:, rows, :], osem.at[e])

    def put(e, width, tiles):
        for w in range(width):
            rows = pl.ds(pl.multiple_of(e * 16 + 8 * w, 8), 8)
            for t in range(3):
                vbuf[:, rows, t * LANES : (t + 1) * LANES] = v_ref[:, rows, t * LANES : (t + 1) * LANES] + tiles[3 * w + t]
            vbuf[:, rows, 3 * LANES : PAIRS] = v_ref[:, rows, 3 * LANES : PAIRS] + rest[:, rows, 0:REST]
        part(e, width).start()

    def load(g):
        return g_ref[:, pl.ds(pl.multiple_of(g * 16, 16), 16), :]

    _step4(lhs_ref, load, put, rest, lane8, True)

    for e in range(TILES // 2):
        part(e, 2).wait()
    part(TILES // 2, 1).wait()


def _last(lhs, g, v):
    return pl.pallas_call(
        _last_kernel,
        out_shape=jax.ShapeDtypeStruct((OCC, VIRT, PAIRS), F32),
        in_specs=[
            pl.BlockSpec(memory_space=pltpu.VMEM),
            pl.BlockSpec(memory_space=pltpu.VMEM),
            pl.BlockSpec(memory_space=pltpu.VMEM),
        ],
        out_specs=pl.BlockSpec(memory_space=pl.ANY),
        scratch_shapes=[
            pltpu.VMEM((OCC, VIRT, PAIRS), F32),
            pltpu.VMEM((OCC, VIRT, LANES), F32),
            pltpu.SemaphoreType.DMA((TILES // 2 + 1,)),
        ],
        compiler_params=pltpu.CompilerParams(vmem_limit_bytes=30 * 1024 * 1024),
        name="last",
    )(lhs, g, v)


def solution(mesh):
    def local_part(ao_rows, occ_coef, virt_coef):
        v, g, lhs = _exchange(ao_rows, pltpu.with_memory_space_constraint(occ_coef.T, pltpu.HBM), pltpu.with_memory_space_constraint(virt_coef, pltpu.HBM))
        return _last(lhs, g, v)

    return jax.shard_map(
        local_part,
        mesh=mesh,
        in_specs=(P(("frag", "dev"), None, None, None), P("frag", None), P("frag", None)),
        out_specs=P("frag", None, "dev"),
        check_vma=False,
    )
```

```python
import functools

import jax
import jax.numpy as jnp
from jax import lax
from jax.experimental import pallas as pl
from jax.experimental.pallas import tpu as pltpu
from jax.sharding import PartitionSpec as P

F32 = jnp.float32
BF16 = jnp.bfloat16
AO, OCC, VIRT = 152, 33, 104
DEVS = 8
ROWS = AO // DEVS
PAIRS = OCC * VIRT // DEVS
PITCH = 41
CHUNK = 19
CHUNKS = AO // CHUNK
SLOTS = 4
RING = 10
LANES = 128
TILES = VIRT // 8
REST = PAIRS - 3 * LANES
RTILES = -(-TILES * REST // LANES)
BLK = 8 * (3 * TILES + RTILES)
GROUPS = ((0, 1, 2, 3, 4, 5), (6, 7, 8, 9, 10, 11, 12, 13), (14, 15, 16, 17, 18, 19, 20, 21), (22, 23, 24, 25, 26, 27, 28, 29, 30, 31, 32))
ORDER = (0, 2, 4, 6, 1, 3, 5, 7)
EARLY = 17
LATE = ROWS - EARLY


def _step4(lhs_ref, load, put, rest, lane8, unroll):
    depth = lhs_ref.shape[1]

    def group(g):
        return load(g).reshape(depth, LANES)

    def product(groups):
        rhs = jnp.concatenate([group(g) for g in groups], axis=1)
        return jnp.dot(lhs_ref[...], rhs, preferred_element_type=F32).reshape(OCC, 16, len(groups) * LANES)

    def tile(v, m):
        g, u = divmod(m, 2)
        return v[:, 8 * u : 8 * u + 8, g * LANES : (g + 1) * LANES]

    base = 18
    v = product([base + k for k in range(BLK // 16 - base)])
    tail = [tile(v, k) for k in range(3)]
    packed = [tile(v, 3 + k) for k in range(RTILES)]
    for n in range(TILES):
        start = REST * n
        k0, k1 = start // LANES, (start + REST - 1) // LANES
        back = (-start) % LANES
        piece = pltpu.roll(packed[k0], back, axis=2) if back else packed[k0]
        if k1 != k0:
            other = pltpu.roll(packed[k1], back, axis=2)
            piece = jnp.where(lane8 < LANES * k1 - start, piece, other)
        rest[:, 8 * n : 8 * n + 8, :] = piece

    def pair(e, carry):
        v = product([3 * e, 3 * e + 1, 3 * e + 2])
        put(e, 2, [tile(v, m) for m in range(6)])
        return carry

    if unroll:
        for e in range(TILES // 2):
            pair(e, 0)
    else:
        lax.fori_loop(0, TILES // 2, pair, 0)
    put(TILES // 2, 1, tail)


def _spread(cot_f32, width, owner):
    k = lax.broadcasted_iota(jnp.int32, (AO, width), 1)
    p = lax.broadcasted_iota(jnp.int32, (AO, width), 0)
    pick = jnp.where(p == owner(k // 16), 1.0, 0.0).astype(BF16)
    wide = jnp.dot(cot_f32, pick, preferred_element_type=F32)[0:OCC]
    a = lax.broadcasted_iota(jnp.int32, (16, width), 0)
    ka = lax.rem(lax.broadcasted_iota(jnp.int32, (16, width), 1), 16)
    keep = (a == ka)[None]
    return jnp.where(keep, wide[:, None, :], 0.0).reshape(OCC * 16, width).astype(BF16)


def _exchange_kernel(
    a_hbm, cot_hbm, cv_hbm, v_out, g_out, lhs_out,
    abuf, cot, cvp, cvt, ts0, ts1, gsend, grecv, rest, lhs,
    asem, ssem, rsem, csem, cot_ref, cv_ref,
):
    me = lax.axis_index("dev")

    def a_copy(n):
        return pltpu.make_async_copy(
            a_hbm.at[n // CHUNKS, pl.ds(lax.rem(n, CHUNKS) * CHUNK, CHUNK)],
            abuf.at[lax.rem(n, SLOTS)],
            asem.at[lax.rem(n, SLOTS)],
        )

    cot_copy = pltpu.make_async_copy(cot_hbm, cot_ref, csem.at[0])
    cv_copy = pltpu.make_async_copy(cv_hbm, cv_ref, csem.at[1])
    cot_copy.start()
    cv_copy.start()
    for n in range(SLOTS):
        a_copy(n).start()

    barrier = pltpu.get_barrier_semaphore()
    for k in range(1, DEVS):
        pl.semaphore_signal(
            barrier, inc=1, device_id={"dev": lax.rem(me + k, DEVS)}, device_id_type=pl.DeviceIdType.MESH
        )

    cot_copy.wait()
    cv_copy.wait()
    cot[...] = jnp.zeros_like(cot)
    cot[0:OCC, :] = cot_ref[...]
    cvp[...] = jnp.zeros_like(cvp)
    cvp[:, 0:VIRT] = cv_ref[...]
    square = jnp.concatenate([cvp[...].astype(F32), jnp.zeros((2 * LANES - AO, LANES), F32)], axis=0)
    cvt[...] = square.T[0:VIRT, 0:AO].astype(BF16)

    lane = lax.broadcasted_iota(jnp.int32, (VIRT, LANES), 1)
    lane8 = lax.broadcasted_iota(jnp.int32, (8, LANES), 1)

    def early_copy(row, src, dst):
        return pltpu.make_async_remote_copy(
            src_ref=gsend.at[lax.rem(row, RING), dst],
            dst_ref=grecv.at[src * EARLY + row],
            send_sem=ssem.at[row, dst],
            recv_sem=rsem.at[row, src],
            device_id={"dev": dst},
            device_id_type=pl.DeviceIdType.MESH,
        )

    def late_copy(row, src, dst, sems=None):
        sems = row if sems is None else sems
        return pltpu.make_async_remote_copy(
            src_ref=gsend.at[lax.rem(row, RING), dst],
            dst_ref=g_out.at[src * LATE + row - EARLY],
            send_sem=ssem.at[sems, dst],
            recv_sem=rsem.at[sems, src],
            device_id={"dev": dst},
            device_id_type=pl.DeviceIdType.MESH,
        )

    def send(row, d):
        @pl.when((d != me) & (row < EARLY))
        def _():
            early_copy(row, me, d).start()

        @pl.when((d != me) & (row >= EARLY))
        def _():
            late_copy(row, me, d).start()

        @pl.when((d == me) & (row < EARLY))
        def _():
            grecv[me * EARLY + row] = gsend[lax.rem(row, RING), d]

        @pl.when((d == me) & (row >= EARLY))
        def _():
            g_out[me * LATE + row - EARLY] = gsend[lax.rem(row, RING), d]

    def sent(row):
        for k in range(DEVS):
            @pl.when(k != me)
            def _():
                late_copy(EARLY, me, k, row).wait_send()

    def row_body(row, carry):
        def chunk_body(c, carry):
            n = row * CHUNKS + c
            slot = lax.rem(n, SLOTS)
            a_copy(n).wait()
            for u in range(CHUNK):
                t = jnp.dot(cot[...], abuf[slot, u], preferred_element_type=F32)
                base = (c * CHUNK + u) * PITCH
                ts0[pl.ds(base, 40), :] = t[:, 0:LANES]
                ts1[pl.ds(base, 40), 0 : AO - LANES] = t[:, LANES:AO]

            @pl.when(n + SLOTS < ROWS * CHUNKS)
            def _():
                a_copy(n + SLOTS).start()

            return carry

        lax.fori_loop(0, CHUNKS, chunk_body, 0)

        @pl.when(row == 0)
        def _():
            pl.semaphore_wait(barrier, DEVS - 1)

        @pl.when(row >= RING)
        def _():
            sent(row - RING)


        g = {}

        def need(j):
            if j in g:
                return
            group = next(js for js in GROUPS if j in js)
            lhs = jnp.concatenate(
                [
                    jnp.concatenate([(ts0, ts1)[k][pl.ds(jj, AO, stride=PITCH), :] for jj in group], axis=0)
                    for k in range(2)
                ],
                axis=1,
            )
            lhs = lhs[:, 0:AO].astype(BF16)
            half = jnp.dot(lhs, cvp[...], preferred_element_type=F32)
            wide = jnp.concatenate([half[AO * n : AO * n + AO] for n in range(len(group))], axis=1).astype(BF16)
            full = jnp.dot(cvt[...], wide, preferred_element_type=F32)
            for n, jj in enumerate(group):
                g[jj] = full[:, LANES * n : LANES * n + LANES]

        for at, d in enumerate(ORDER):
            first = PAIRS * d
            j0, j1 = first // VIRT, (first + PAIRS - 1) // VIRT
            rolled = {}
            for j in range(j0, j1 + 1):
                need(j)
                shift = (VIRT * j - first) % LANES
                rolled[j] = pltpu.roll(g[j], shift, axis=1) if shift else g[j]
            tiles = []
            for t in range(4):
                lo = first + LANES * t
                hi = min(lo + LANES, first + PAIRS)
                ja, jb = lo // VIRT, (hi - 1) // VIRT
                tile = rolled[ja]
                for j in range(ja + 1, jb + 1):
                    tile = jnp.where(lane >= VIRT * j - lo, rolled[j], tile)
                tiles.append(tile)
            last = tiles.pop()
            parts = [tile[8 * n : 8 * n + 8] for n in range(TILES) for tile in tiles]
            moved = []
            for n in range(TILES):
                shift = REST * n % LANES
                piece = last[8 * n : 8 * n + 8]
                moved.append(pltpu.roll(piece, shift, axis=1) if shift else piece)
            for k in range(RTILES):
                n0, n1 = LANES * k // REST, min((LANES * k + LANES - 1) // REST, TILES - 1)
                part = moved[n0]
                for n in range(n0 + 1, n1 + 1):
                    part = jnp.where(lane8 >= REST * n - LANES * k, moved[n], part)
                parts.append(part)
            gsend[lax.rem(row, RING), d] = jnp.concatenate(parts, axis=0).astype(BF16)
            if at:
                send(row, ORDER[at - 1])
        send(row, ORDER[-1])
        return carry

    lax.fori_loop(0, ROWS, row_body, 0)

    v_out[...] = jnp.zeros_like(v_out)
    for s in range(DEVS):
        cols = slice(s * EARLY * 16, (s + 1) * EARLY * 16)
        lhs[:, cols] = _spread(cot[...], EARLY * 16, lambda q: s * ROWS + q)
    lhs_out[...] = _spread(cot[...], DEVS * LATE * 16, lambda q: q // LATE * ROWS + EARLY + lax.rem(q, LATE))

    def arrived(row, carry):
        for k in range(DEVS):
            @pl.when(k != me)
            def _():
                early_copy(row, k, me).wait_recv()

        return carry

    lax.fori_loop(0, EARLY, arrived, 0)

    def put(e, width, tiles):
        for w in range(width):
            rows = pl.ds(pl.multiple_of(e * 16 + 8 * w, 8), 8)
            for t in range(3):
                v_out[:, rows, t * LANES : (t + 1) * LANES] += tiles[3 * w + t]
            v_out[:, rows, 3 * LANES : PAIRS] = rest[:, rows, 0:REST]

    def load(g):
        return grecv[:, pl.ds(pl.multiple_of(g * 16, 16), 16), :]

    _step4(lhs, load, put, rest, lane8, False)

    def arrived_late(row, carry):
        for k in range(DEVS):
            @pl.when(k != me)
            def _():
                late_copy(row, k, me).wait_recv()

        return carry

    lax.fori_loop(EARLY, ROWS, arrived_late, 0)

    lax.fori_loop(ROWS - RING, ROWS, lambda row, carry: sent(row) or carry, 0)


def _exchange(ao_rows, cot, cv):
    return pl.pallas_call(
        _exchange_kernel,
        out_shape=(
            jax.ShapeDtypeStruct((OCC, VIRT, PAIRS), F32),
            jax.ShapeDtypeStruct((DEVS * LATE, BLK, LANES), BF16),
            jax.ShapeDtypeStruct((OCC * 16, DEVS * LATE * 16), BF16),
        ),
        in_specs=[pl.BlockSpec(memory_space=pltpu.HBM)] * 3,
        out_specs=tuple(pl.BlockSpec(memory_space=pltpu.VMEM) for _ in range(3)),
        scratch_shapes=[
            pltpu.VMEM((SLOTS, CHUNK, AO, AO), BF16),
            pltpu.VMEM((40, AO), BF16),
            pltpu.VMEM((AO, LANES), BF16),
            pltpu.VMEM((VIRT, AO), BF16),
            pltpu.VMEM((AO * PITCH, LANES), F32),
            pltpu.VMEM((AO * PITCH, LANES), F32),
            pltpu.VMEM((RING, DEVS, BLK, LANES), BF16),
            pltpu.VMEM((DEVS * EARLY, BLK, LANES), BF16),
            pltpu.VMEM((OCC, VIRT, LANES), F32),
            pltpu.VMEM((OCC * 16, DEVS * EARLY * 16), BF16),
            pltpu.SemaphoreType.DMA((SLOTS,)),
            pltpu.SemaphoreType.DMA((ROWS, DEVS)),
            pltpu.SemaphoreType.DMA((ROWS, DEVS)),
            pltpu.SemaphoreType.DMA((2,)),
            pltpu.VMEM((OCC, AO), BF16),
            pltpu.VMEM((AO, VIRT), BF16),
        ],
        compiler_params=pltpu.CompilerParams(
            collective_id=0, has_side_effects=True, vmem_limit_bytes=38 * 1024 * 1024
        ),
        name="exchange",
    )(ao_rows, cot, cv)


def _last_kernel(lhs_ref, g_ref, v_ref, out_hbm, vbuf, rest, osem):
    lane8 = lax.broadcasted_iota(jnp.int32, (8, LANES), 1)

    def part(e, width):
        rows = pl.ds(pl.multiple_of(e * 16, 8), 8 * width)
        return pltpu.make_async_copy(vbuf.at[:, rows, :], out_hbm.at[:, rows, :], osem.at[e])

    def put(e, width, tiles):
        for w in range(width):
            rows = pl.ds(pl.multiple_of(e * 16 + 8 * w, 8), 8)
            for t in range(3):
                vbuf[:, rows, t * LANES : (t + 1) * LANES] = v_ref[:, rows, t * LANES : (t + 1) * LANES] + tiles[3 * w + t]
            vbuf[:, rows, 3 * LANES : PAIRS] = v_ref[:, rows, 3 * LANES : PAIRS] + rest[:, rows, 0:REST]
        part(e, width).start()

    def load(g):
        return g_ref[:, pl.ds(pl.multiple_of(g * 16, 16), 16), :]

    _step4(lhs_ref, load, put, rest, lane8, True)

    for e in range(TILES // 2):
        part(e, 2).wait()
    part(TILES // 2, 1).wait()


def _last(lhs, g, v):
    return pl.pallas_call(
        _last_kernel,
        out_shape=jax.ShapeDtypeStruct((OCC, VIRT, PAIRS), F32),
        in_specs=[
            pl.BlockSpec(memory_space=pltpu.VMEM),
            pl.BlockSpec(memory_space=pltpu.VMEM),
            pl.BlockSpec(memory_space=pltpu.VMEM),
        ],
        out_specs=pl.BlockSpec(memory_space=pl.ANY),
        scratch_shapes=[
            pltpu.VMEM((OCC, VIRT, PAIRS), F32),
            pltpu.VMEM((OCC, VIRT, LANES), F32),
            pltpu.SemaphoreType.DMA((TILES // 2 + 1,)),
        ],
        compiler_params=pltpu.CompilerParams(vmem_limit_bytes=30 * 1024 * 1024),
        name="last",
    )(lhs, g, v)


def solution(mesh):
    def local_part(ao_rows, occ_coef, virt_coef):
        v, g, lhs = _exchange(ao_rows, pltpu.with_memory_space_constraint(occ_coef.T, pltpu.HBM), pltpu.with_memory_space_constraint(virt_coef, pltpu.HBM))
        return _last(lhs, g, v)

    return jax.shard_map(
        local_part,
        mesh=mesh,
        in_specs=(P(("frag", "dev"), None, None, None), P("frag", None), P("frag", None)),
        out_specs=P("frag", None, "dev"),
        check_vma=False,
    )
```
